32 devices in a mesh: row: 4 (over y, core), col: 8 (over z, x).
Axes of the slice: x: 2, y: 2, z: 4, core: 2. Of those that a mesh axis runs over, the one named last changes fastest.
Arguments:
- root_inverse: bfloat16 [2048, 2048], P('col', 'row'), may hold values from -1 to 3, as said below
- lower_panels: bfloat16 [4, 1536, 1024], P(None, 'col', 'row'), may hold values from -0.375 to 0.375
- struct_blocks: int32 [4, 12], replicated, may hold values from 0 to 15, as said below
- struct_count: int32 [4], replicated, may hold values from 1 to 12, 32 in all
- diag_inverse: float32 [4, 1024, 1024], P(None, 'col', 'row'), may hold values from -1 to 3, as said below
Outputs:
- offdiag: bfloat16 [4, 1536, 1024], P(None, 'col', 'row')
- diag_block: float32 [4, 1024, 1024], P(None, 'col', 'row')
The draws below stay inside these ranges and needn't reach their ends.
Inputs may be any that keep to these rules, and one draw needn't show every extreme that they name: `struct_blocks`: each row holds 12 different block numbers of the top supernode; supernode c uses the first struct_count[c] of them. `struct_count`: the counts sum to 32; the largest equals 12. `root_inverse`: Symmetric, with a dominant diagonal. `diag_inverse`: each supernode's block is symmetric; diagonal entries lie between 0.85 and 2.15, all other entries within 0.13 of zero.
All inputs are finite; a program needn't handle non-finite values.
Results may differ from the reference program's by a relative error of at most 0.0095.
Values may be sent and summed in bfloat16 or wider, within the bound.
A program may use at most 64 MiB of HBM per device.

```python
import math
import jax
import jax.numpy as jnp
import numpy as np
from jax import lax

W = 2048
W1 = 1024
BLOCK = 128
NSMAX = 12
K = 4


def symmetric_batch(seed_key, batch_count, matrix_order):
    noise = jnp.clip(jax.random.normal(seed_key, (batch_count, matrix_order, matrix_order)), -4.0, 4.0)
    mixed = (noise + jnp.swapaxes(noise, 1, 2)) * (0.5 / math.sqrt(matrix_order))
    diagonal_part = jax.random.uniform(jax.random.fold_in(seed_key, 7), (batch_count, matrix_order, 1), minval=1.0, maxval=2.0)
    return mixed + diagonal_part * jnp.eye(matrix_order, dtype=jnp.float32)


def draw_root_inverse(key, part):
    return symmetric_batch(jax.random.fold_in(key, 11), 1, W)[0].astype(jnp.bfloat16)


def draw_diag_inverse(key, part):
    return symmetric_batch(jax.random.fold_in(key, 13), K, W1)


def draw_struct_blocks(key, part):
    subkeys = jax.random.split(jax.random.fold_in(key, 17), K)
    chosen = jax.vmap(lambda one_key: jax.random.permutation(one_key, W // BLOCK)[:NSMAX])(subkeys)
    return chosen.astype(jnp.int32)


def block_levels(stream_key, extent, cuts, low, high):
    def one(dim, parts):
        draws = jax.random.uniform(jax.random.fold_in(jax.random.fold_in(stream_key, 6), dim), (parts,), jnp.float32, low / len(cuts), high / len(cuts))
        return jnp.repeat(jnp.exp(draws), extent[dim] // parts).reshape((-1,) + (1,) * (len(extent) - dim - 1))

    loudness = one(*cuts[0])
    for cut in cuts[1:]:
        loudness = loudness * one(*cut)
    return loudness


def split_up(amount, total, most, lean):
    weights = [(1 << 20) // math.isqrt(standing ** lean) + 1 for standing in range(2, amount + 1)]
    rest, given = total - most - (amount - 1), [1] * (amount - 1)
    while rest > 0:
        free = [i for i in range(amount - 1) if given[i] < most]
        pool, left = sum([weights[i] for i in free]), rest
        for i in free:
            addition = min(most - given[i], max(1, left * weights[i] // pool), rest)
            given[i] = given[i] + addition
            rest = rest - addition
    return np.array([most] + given)


def ragged_sizes(rng, number_of, total, bound, lean):
    if number_of == 2:
        one = jax.random.randint(rng, (), max(1, total - bound), min(bound, total - 1) + 1)
        return jnp.stack([one, total - one])
    sizes = jnp.asarray(split_up(number_of, total, bound, lean), jnp.int32)
    pairs = (number_of - 1) // 2
    giver, taker = sizes[1:1 + 2 * pairs:2], sizes[2:2 + 2 * pairs:2]
    margin = jnp.minimum(giver - 1, bound - taker)
    passed = jax.random.randint(jax.random.fold_in(rng, 1), (pairs,), 0, 1 << 20) % (margin + 1)
    sizes = sizes.at[1:1 + 2 * pairs:2].set(giver - passed).at[2:2 + 2 * pairs:2].set(taker + passed)
    return sizes[jax.random.permutation(jax.random.fold_in(rng, 2), number_of)]


def gaussian(own_key, shape, deviation, bound, shards=(), held_as=jnp.bfloat16):
    array = deviation * jax.random.normal(own_key, shape, jnp.float32)
    if shards:
        array = array * block_levels(own_key, shape, shards, -0.22, 0.18)
    return jnp.clip(array, -bound, bound).astype(held_as)


def setup_inputs(seed: int = 0) -> dict:
    key_of = jax.random.split(jax.random.key(seed), 6)
    root_inverse = draw_root_inverse(jax.random.fold_in(key_of[5], 71), 0)
    lower_panels = gaussian(key_of[1], (K, NSMAX * BLOCK, W1), 256 ** -0.5, 0.375, ((1, 8), (2, 4)))
    struct_blocks = draw_struct_blocks(jax.random.fold_in(key_of[5], 71), 0)
    struct_count = ragged_sizes(key_of[3], K, K * 8, NSMAX, 2).astype(jnp.int32)
    diag_inverse = draw_diag_inverse(jax.random.fold_in(key_of[5], 71), 0)
    return {"root_inverse": root_inverse, "lower_panels": lower_panels, "struct_blocks": struct_blocks, "struct_count": struct_count, "diag_inverse": diag_inverse}


def reference(root_inverse, lower_panels, struct_blocks, struct_count, diag_inverse):
    block_count = W // BLOCK
    root_blocks = root_inverse.reshape(block_count, BLOCK, block_count, BLOCK)

    def one_child(child_inputs):
        lower_panel, block_list, used_count, diag_inv = child_inputs
        in_use = (jnp.arange(NSMAX) < used_count).astype(jnp.float32)
        row_mask = jnp.repeat(in_use, BLOCK)
        masked = lower_panel * row_mask.astype(jnp.bfloat16)[:, None]
        ancestors = root_blocks[block_list][:, :, block_list, :].reshape(NSMAX * BLOCK, NSMAX * BLOCK)
        product = jnp.dot(ancestors, masked, preferred_element_type=jnp.float32)
        offdiag = (-product * row_mask[:, None]).astype(jnp.bfloat16)
        schur_part = jnp.dot(masked.T, offdiag, preferred_element_type=jnp.float32)
        return offdiag, diag_inv - schur_part

    offdiag, diag_block = lax.map(one_child, (lower_panels, struct_blocks, struct_count, diag_inverse))
    return (offdiag, diag_block)
```

```python
import functools

import jax
import jax.numpy as jnp
from jax import lax
from jax.experimental import pallas as pl
from jax.experimental.pallas import tpu as pltpu
from jax.sharding import PartitionSpec as P

BLOCK = 128
NSMAX = 12


def body(root_inverse, lower_panels, struct_blocks, struct_count, diag_inverse):
    col_index = lax.axis_index("col")
    root_panel = lax.all_gather(root_inverse, "row", axis=1, tiled=True)
    root_width = root_panel.shape[1]
    block_count = root_width // BLOCK
    own_rows = root_panel.shape[0]
    per_dev = own_rows // BLOCK
    local_packed = lower_panels.shape[1]

    def solve_group(lower_group, block_lists, block_counts, inverse_group):
        group_size = lower_group.shape[0]
        cols_here = lower_group.shape[2]
        gathered = lax.all_gather(lower_group, "col", axis=1, tiled=True)
        packed_total = gathered.shape[1]
        full_mask = jnp.arange(packed_total)[None, :] // BLOCK < block_counts[:, None]
        gathered = gathered * full_mask[:, :, None].astype(jnp.bfloat16)
        in_use = jnp.arange(NSMAX)[None, :] < block_counts[:, None]
        onehot = (
            (block_lists[:, None, :] == jnp.arange(block_count)[None, :, None]) & in_use[:, None, :]
        ).astype(jnp.bfloat16)
        spread = jnp.einsum(
            "gbk,gkic->gbic",
            onehot,
            gathered.reshape(group_size, NSMAX, BLOCK, cols_here),
            preferred_element_type=jnp.float32,
        )
        spread = spread.astype(jnp.bfloat16).reshape(group_size, root_width, cols_here)
        root_part = -jnp.einsum(
            "rw,gwc->grc", root_panel, spread, preferred_element_type=jnp.float32
        )
        packed_index = col_index * local_packed + jnp.arange(local_packed)
        local_mask = packed_index[None, :] // BLOCK < block_counts[:, None]
        own_select = lax.dynamic_slice_in_dim(onehot, col_index * per_dev, per_dev, 1).astype(
            jnp.float32
        )
        selected = jnp.einsum(
            "gjk,gjic->gkic",
            own_select,
            root_part.reshape(group_size, per_dev, BLOCK, cols_here),
            precision=lax.Precision.HIGHEST,
            preferred_element_type=jnp.float32,
        )
        selected = selected.reshape(group_size, packed_total, cols_here)
        offdiag = lax.psum_scatter(
            selected.astype(jnp.bfloat16), "col", scatter_dimension=1, tiled=True
        )
        full_cols = lax.all_gather(lower_group, "row", axis=2, tiled=True)
        masked_rows = full_cols * local_mask[:, :, None].astype(jnp.bfloat16)
        schur_terms = jnp.einsum(
            "gka,gkc->gac", masked_rows, offdiag, preferred_element_type=jnp.float32
        )
        schur_part = lax.psum_scatter(
            schur_terms.astype(jnp.bfloat16), "col", scatter_dimension=1, tiled=True
        ).astype(jnp.float32)
        return (offdiag, inverse_group - schur_part)

    group_size = 4
    turn_count = lower_panels.shape[0] // group_size

    def regroup(source_array):
        return source_array.reshape((turn_count, group_size) + source_array.shape[1:])

    def one_turn(running, inputs_now):
        return (running, solve_group(*inputs_now))

    finished, outputs = lax.scan(
        one_turn,
        jnp.int32(0),
        (
            regroup(lower_panels),
            regroup(struct_blocks),
            regroup(struct_count),
            regroup(diag_inverse),
        ),
    )
    offdiag_all, diag_all = outputs
    return (offdiag_all.reshape(lower_panels.shape), diag_all.reshape(diag_inverse.shape))


def place(slices):
    row, col = lax.axis_index("row"), lax.axis_index("col")
    return row // 2, row % 2, col // 2, col % 2


def at(y, core, z, x):
    return {"row": 2 * y + core, "col": 2 * z + x}


def greet(peers):
    barrier = pltpu.get_barrier_semaphore()
    for peer in peers:
        pl.semaphore_signal(barrier, inc=1, device_id=peer, device_id_type=pl.DeviceIdType.MESH)
    pl.semaphore_wait(barrier, len(peers))


def send(src, dst, send_sem, recv_sem, device):
    return pltpu.make_async_remote_copy(
        src_ref=src,
        dst_ref=dst,
        send_sem=send_sem,
        recv_sem=recv_sem,
        device_id=device,
        device_id_type=pl.DeviceIdType.MESH,
    )


def gather_kernel(slices, root_ref, panel_ref, half_ref, quad_ref, own_ref, side_ref, *sems):
    (zr_s, zr_r, zp_s, zp_r, xr_s, xr_r, xp_s, xp_r, yr_s, yr_r, yp_s, yp_r, hc_s, hc_r, qc_s, qc_r, pc_s, pc_r, loc) = sems
    y, core, z, x = place(slices)
    width = root_ref.shape[1]
    chunk = 2 * slices
    lanes = pl.ds(pl.multiple_of(core * width, width), width)
    part = side_ref.shape[3]
    x_peer, y_peer, c_peer = at(y, core, z, 1 - x), at(1 - y, core, z, x), at(y, 1 - core, z, x)

    def z_at(d):
        return lax.rem(z + d, slices)

    z_peers = [at(y, core, z_at(d), x) for d in range(1, slices)]
    greet(z_peers + [x_peer, y_peer, c_peer])

    def half_piece(zz, xx):
        return half_ref.at[lax.rem(2 * zz + xx + slices * y, chunk), :, lanes]

    def quad_piece(zz, xx):
        return quad_ref.at[2 * lax.rem(zz, slices // 2) + xx, :, lanes]

    def own_piece(zz, xx):
        return own_ref.at[2 * zz + xx]

    def in_quad(zz):
        return zz // (slices // 2) == y

    def z_panel(d):
        return send(panel_ref.at[z_at(d)], own_piece(z, x), zp_s.at[d], zp_r.at[d], at(y, core, z_at(d), x))

    def z_root(d):
        return send(root_ref, half_piece(z, x), zr_s.at[d], zr_r.at[d], at(y, core, z_at(d), x))

    def back(d):
        return lax.rem(z + slices - d, slices)

    def x_panel(d):
        src = panel_ref.at[z] if d == 0 else own_piece(back(d), x)
        return send(src, own_piece(back(d), x), xp_s.at[d], xp_r.at[d], x_peer)

    def x_root(d):
        src = root_ref if d == 0 else half_piece(back(d), x)
        return send(src, half_piece(back(d), x), xr_s.at[d], xr_r.at[d], x_peer)

    def y_root(zz, xx, src):
        index = 2 * lax.rem(zz, slices // 2) + xx
        return send(src, quad_ref.at[index, :, lanes], yr_s.at[index], yr_r.at[index], y_peer)

    def c_half(slot, zz, xx, src):
        return send(src, half_piece(zz, xx), hc_s.at[slot], hc_r.at[slot], c_peer)

    def c_quad(index):
        return send(quad_ref.at[index, :, lanes], quad_ref.at[index, :, lanes], qc_s.at[index], qc_r.at[index], c_peer)

    my_side = own_ref.at[:, :, pl.ds(pl.multiple_of(x * part, part), part)]

    def side_slot(yy, cc):
        return side_ref.at[2 * yy + cc]

    y_side = send(my_side, side_slot(y, core), yp_s, yp_r, y_peer)
    c_side = [
        send(my_side, side_slot(y, core), pc_s.at[0], pc_r.at[0], c_peer),
        send(side_slot(1 - y, core), side_slot(1 - y, core), pc_s.at[1], pc_r.at[1], c_peer),
    ]

    for d in range(1, slices):
        z_panel(d).start()
    x_panel(0).start()
    for d in range(1, slices):
        z_root(d).start()
    x_root(0).start()

    @pl.when(in_quad(z))
    def _():
        y_root(z, x, root_ref).start()

    c_half(0, z, x, root_ref).start()
    local = [
        pltpu.make_async_copy(root_ref, half_piece(z, x), loc.at[0]),
        pltpu.make_async_copy(panel_ref.at[z], own_piece(z, x), loc.at[1]),
    ]
    for copy in local:
        copy.start()
    for d in range(1, slices):
        z_panel(d).wait_recv()
        x_panel(d).start()
    local[1].wait()
    for d in range(slices):
        x_panel(d).wait_recv()
    y_side.start()
    c_side[0].start()
    own_side = pltpu.make_async_copy(my_side, side_slot(y, core), loc.at[2])
    own_side.start()

    def spread_on(slot, zz, xx):
        @pl.when(in_quad(zz))
        def _():
            y_root(zz, xx, half_piece(zz, xx)).start()

        c_half(slot, zz, xx, half_piece(zz, xx)).start()

    x_root(0).wait_recv()
    spread_on(slices, z, 1 - x)
    for d in range(1, slices):
        z_root(d).wait_recv()
        x_root(d).start()
        spread_on(d, back(d), x)
    for d in range(1, slices):
        x_root(d).wait_recv()
        spread_on(slices + d, back(d), 1 - x)
    y_side.wait_recv()
    c_side[1].start()
    for index in range(slices):
        send(root_ref, quad_ref.at[index, :, lanes], yr_s.at[index], yr_r.at[index], y_peer).wait_recv()
        c_quad(index).start()
    for slot in range(2 * slices):
        c_half(slot, z, x, root_ref).wait_recv()
    for index in range(slices):
        c_quad(index).wait_recv()
    for copy in c_side:
        copy.wait_recv()
    local[0].wait()
    own_side.wait()
    for d in range(slices):
        if d > 0:
            z_panel(d).wait_send()
            z_root(d).wait_send()
        x_panel(d).wait_send()
        x_root(d).wait_send()
        send(root_ref, quad_ref.at[d, :, lanes], yr_s.at[d], yr_r.at[d], y_peer).wait_send()
        c_quad(d).wait_send()
    for slot in range(2 * slices):
        c_half(slot, z, x, root_ref).wait_send()
    y_side.wait_send()
    for copy in c_side:
        copy.wait_send()


def solve_kernel(list_ref, count_ref, half_ref, quad_ref, own_ref, side_ref, off_ref, schur_ref, spread, product):
    half = half_ref.shape[0] // 2
    tile = 2 * BLOCK
    used = count_ref[0]
    spread[...] = jnp.zeros_like(spread)
    for k in range(NSMAX):

        @pl.when(k < used)
        def _():
            rows = pl.ds(pl.multiple_of(list_ref[k] * BLOCK, BLOCK), BLOCK)
            spread[rows, :] = own_ref[pl.ds(k * BLOCK, BLOCK), :]

    near, far = spread[:half, :], spread[half:, :]

    def step(t, carry):
        rows = pl.ds(pl.multiple_of(t * tile, tile), tile)
        low = pl.ds(pl.multiple_of(half + t * tile, tile), tile)
        product[rows, :] = jnp.dot(
            half_ref[rows, :], near, preferred_element_type=jnp.float32
        ) + lax.dot_general(
            half_ref[pl.ds(half, half), rows], far, (((0,), (0,)), ((), ())), preferred_element_type=jnp.float32
        )
        product[low, :] = jnp.dot(
            half_ref[low, :], near, preferred_element_type=jnp.float32
        ) + jnp.dot(quad_ref[rows, :], far, preferred_element_type=jnp.float32)
        return carry

    lax.fori_loop(0, half // tile, step, 0)
    for k in range(NSMAX):
        rows = pl.ds(pl.multiple_of(list_ref[k] * BLOCK, BLOCK), BLOCK)
        off_ref[pl.ds(k * BLOCK, BLOCK), :] = jnp.where(k < used, -product[rows, :], 0.0).astype(jnp.bfloat16)
    off = off_ref[...]
    for part in range(side_ref.shape[0]):
        schur_ref[part] = lax.dot_general(
            side_ref[part], off, (((0,), (0,)), ((), ())), preferred_element_type=jnp.float32
        ).astype(jnp.bfloat16)


def return_kernel(slices, off_ref, schur_ref, off_out, schur_out, os, orr, ss, sr, loc):
    y, core, z, x = place(slices)

    def target(d):
        return at(y, core, lax.rem(z + d, slices), x)

    greet([target(d) for d in range(1, slices)])
    copies = []
    for d in range(1, slices):
        zz = lax.rem(z + d, slices)
        copies.append(send(off_ref.at[2 * zz + x], off_out.at[z], os.at[d], orr.at[d], target(d)))
    for d in range(1, slices):
        zz = lax.rem(z + d, slices)
        copies.append(send(schur_ref.at[zz], schur_out.at[z], ss.at[d], sr.at[d], target(d)))
    for copy in copies:
        copy.start()
    local = [
        pltpu.make_async_copy(off_ref.at[2 * z + x], off_out.at[z], loc.at[0]),
        pltpu.make_async_copy(schur_ref.at[z], schur_out.at[z], loc.at[1]),
    ]
    for copy in local:
        copy.start()
    for copy in local + copies:
        copy.wait()


def owner_body(slices, root_inverse, lower_panels, struct_blocks, struct_count, diag_inverse):
    y, core, z, x = place(slices)
    vmem = pl.BlockSpec(memory_space=pltpu.VMEM)
    smem = pl.BlockSpec(memory_space=pltpu.SMEM)
    bf16 = jnp.bfloat16
    root_rows, root_cols = root_inverse.shape
    count, local_rows, local_cols = lower_panels.shape
    chunk = 2 * slices
    order = root_rows * chunk
    part = local_cols // 2
    dma = pltpu.SemaphoreType.DMA
    pair = lambda n: [dma((n,)), dma((n,))]
    one = [dma, dma]
    half, quad, own, side = pl.pallas_call(
        functools.partial(gather_kernel, slices),
        out_shape=[
            jax.ShapeDtypeStruct((chunk, root_rows, 2 * root_cols), bf16),
            jax.ShapeDtypeStruct((slices, root_rows, 2 * root_cols), bf16),
            jax.ShapeDtypeStruct((chunk, local_rows, local_cols), bf16),
            jax.ShapeDtypeStruct((4, chunk, local_rows, part), bf16),
        ],
        in_specs=[vmem] * 2,
        out_specs=[vmem] * 4,
        scratch_shapes=pair(slices) * 4 + pair(slices) + one + pair(2 * slices) + pair(slices) + pair(2) + [dma((3,))],
        compiler_params=pltpu.CompilerParams(collective_id=0, has_side_effects=True),
    )(root_inverse, lower_panels)
    blocks = order // BLOCK
    mine = lax.dynamic_index_in_dim(struct_blocks, z, 0, keepdims=False)
    listed = lax.rem(mine + y * (blocks // 2), blocks)
    used = lax.dynamic_slice_in_dim(struct_count, z, 1, 0)
    packed = chunk * local_rows
    off, schur = pl.pallas_call(
        solve_kernel,
        out_shape=[
            jax.ShapeDtypeStruct((packed, local_cols), bf16),
            jax.ShapeDtypeStruct((4, part, local_cols), bf16),
        ],
        in_specs=[smem] * 2 + [vmem] * 4,
        out_specs=[vmem] * 2,
        scratch_shapes=[pltpu.VMEM((order, local_cols), bf16), pltpu.VMEM((order, local_cols), jnp.float32)],
    )(
        listed,
        used,
        half.reshape(order, 2 * root_cols),
        quad.reshape(order // 2, 2 * root_cols),
        own.reshape(packed, local_cols),
        side.reshape(4, packed, part),
    )
    offdiag, terms = pl.pallas_call(
        functools.partial(return_kernel, slices),
        out_shape=[
            jax.ShapeDtypeStruct(lower_panels.shape, bf16),
            jax.ShapeDtypeStruct((count, part, local_cols), bf16),
        ],
        in_specs=[vmem] * 2,
        out_specs=[vmem] * 2,
        scratch_shapes=pair(slices) * 2 + [dma((2,))],
        compiler_params=pltpu.CompilerParams(collective_id=1, has_side_effects=True),
    )(off.reshape(chunk, local_rows, local_cols), schur)
    return (offdiag, diag_inverse - terms.astype(jnp.float32))


def spread_body(*arguments):
    rows, cols = lax.axis_size("row"), lax.axis_size("col")
    slices = arguments[1].shape[0]
    if cols == 2 * slices and rows == 4 and slices == 4:
        return owner_body(slices, *arguments)
    return body(*arguments)


def solution(mesh):
    in_specs = (P("col", "row"), P(None, "col", "row"), P(), P(), P(None, "col", "row"))
    out_specs = (P(None, "col", "row"), P(None, "col", "row"))
    return jax.shard_map(spread_body, mesh=mesh, in_specs=in_specs, out_specs=out_specs, check_vma=False)
```

```python
import functools

import jax
import jax.numpy as jnp
from jax import lax
from jax.experimental import pallas as pl
from jax.experimental.pallas import tpu as pltpu
from jax.sharding import PartitionSpec as P

BLOCK = 128
NSMAX = 12


def body(root_inverse, lower_panels, struct_blocks, struct_count, diag_inverse):
    col_index = lax.axis_index("col")
    root_panel = lax.all_gather(root_inverse, "row", axis=1, tiled=True)
    root_width = root_panel.shape[1]
    block_count = root_width // BLOCK
    own_rows = root_panel.shape[0]
    per_dev = own_rows // BLOCK
    local_packed = lower_panels.shape[1]

    def solve_group(lower_group, block_lists, block_counts, inverse_group):
        group_size = lower_group.shape[0]
        cols_here = lower_group.shape[2]
        gathered = lax.all_gather(lower_group, "col", axis=1, tiled=True)
        packed_total = gathered.shape[1]
        full_mask = jnp.arange(packed_total)[None, :] // BLOCK < block_counts[:, None]
        gathered = gathered * full_mask[:, :, None].astype(jnp.bfloat16)
        in_use = jnp.arange(NSMAX)[None, :] < block_counts[:, None]
        onehot = (
            (block_lists[:, None, :] == jnp.arange(block_count)[None, :, None]) & in_use[:, None, :]
        ).astype(jnp.bfloat16)
        spread = jnp.einsum(
            "gbk,gkic->gbic",
            onehot,
            gathered.reshape(group_size, NSMAX, BLOCK, cols_here),
            preferred_element_type=jnp.float32,
        )
        spread = spread.astype(jnp.bfloat16).reshape(group_size, root_width, cols_here)
        root_part = -jnp.einsum(
            "rw,gwc->grc", root_panel, spread, preferred_element_type=jnp.float32
        )
        packed_index = col_index * local_packed + jnp.arange(local_packed)
        local_mask = packed_index[None, :] // BLOCK < block_counts[:, None]
        own_select = lax.dynamic_slice_in_dim(onehot, col_index * per_dev, per_dev, 1).astype(
            jnp.float32
        )
        selected = jnp.einsum(
            "gjk,gjic->gkic",
            own_select,
            root_part.reshape(group_size, per_dev, BLOCK, cols_here),
            precision=lax.Precision.HIGHEST,
            preferred_element_type=jnp.float32,
        )
        selected = selected.reshape(group_size, packed_total, cols_here)
        offdiag = lax.psum_scatter(
            selected.astype(jnp.bfloat16), "col", scatter_dimension=1, tiled=True
        )
        full_cols = lax.all_gather(lower_group, "row", axis=2, tiled=True)
        masked_rows = full_cols * local_mask[:, :, None].astype(jnp.bfloat16)
        schur_terms = jnp.einsum(
            "gka,gkc->gac", masked_rows, offdiag, preferred_element_type=jnp.float32
        )
        schur_part = lax.psum_scatter(
            schur_terms.astype(jnp.bfloat16), "col", scatter_dimension=1, tiled=True
        ).astype(jnp.float32)
        return (offdiag, inverse_group - schur_part)

    group_size = 4
    turn_count = lower_panels.shape[0] // group_size

    def regroup(source_array):
        return source_array.reshape((turn_count, group_size) + source_array.shape[1:])

    def one_turn(running, inputs_now):
        return (running, solve_group(*inputs_now))

    finished, outputs = lax.scan(
        one_turn,
        jnp.int32(0),
        (
            regroup(lower_panels),
            regroup(struct_blocks),
            regroup(struct_count),
            regroup(diag_inverse),
        ),
    )
    offdiag_all, diag_all = outputs
    return (offdiag_all.reshape(lower_panels.shape), diag_all.reshape(diag_inverse.shape))


def place(slices):
    row, col = lax.axis_index("row"), lax.axis_index("col")
    return row // 2, row % 2, col // 2, col % 2


def at(y, core, z, x):
    return {"row": 2 * y + core, "col": 2 * z + x}


def greet(peers):
    barrier = pltpu.get_barrier_semaphore()
    for peer in peers:
        pl.semaphore_signal(barrier, inc=1, device_id=peer, device_id_type=pl.DeviceIdType.MESH)
    pl.semaphore_wait(barrier, len(peers))


def send(src, dst, send_sem, recv_sem, device):
    return pltpu.make_async_remote_copy(
        src_ref=src,
        dst_ref=dst,
        send_sem=send_sem,
        recv_sem=recv_sem,
        device_id=device,
        device_id_type=pl.DeviceIdType.MESH,
    )


SUB = 2


def gather_kernel(slices, root_ref, panel_ref, half_ref, quad_ref, own_ref, side_ref, *sems):
    (zo_s, zr_s, zr_r, zp_s, zp_r, xr_s, xr_r, xp_s, xp_r, yr_s, yr_r, yp_s, yp_r, hc_s, hc_r, qc_s, qc_r, pc_s, pc_r, loc) = sems
    y, core, z, x = place(slices)
    height, width = root_ref.shape[0] // SUB, root_ref.shape[1]
    chunk = 2 * slices
    middle = slices // 2
    lanes = pl.ds(pl.multiple_of(core * width, width), width)
    part = side_ref.shape[3]
    x_peer, y_peer, c_peer = at(y, core, z, 1 - x), at(1 - y, core, z, x), at(y, 1 - core, z, x)

    def z_at(d):
        return lax.rem(z + d, slices)

    def back(d):
        return lax.rem(z + slices - d, slices)

    greet([at(y, core, z_at(d), x) for d in range(1, slices)] + [x_peer, y_peer, c_peer])

    def rows(s):
        return pl.ds(s * height, height)

    def root_piece(s):
        return root_ref.at[rows(s)]

    def half_piece(zz, xx, s):
        return half_ref.at[lax.rem(2 * zz + xx + slices * y, chunk), rows(s), lanes]

    def own_piece(zz, xx):
        return own_ref.at[2 * zz + xx]

    def z_own(way, s):
        step = 1 - 2 * way
        return send(
            root_piece(s), half_piece(z, x, s), zo_s.at[way * SUB + s], zr_r.at[z * SUB + s], at(y, core, z + step, x)
        )

    def z_pass(zz, s, step):
        piece = half_piece(zz, x, s)
        return send(piece, piece, zr_s.at[zz * SUB + s], zr_r.at[zz * SUB + s], at(y, core, z + step, x))

    def when_passed(zz, action):
        above = (zz + slices - z) // slices

        @pl.when((above == 0) & (z < slices - 1))
        def _():
            action(1)

        @pl.when((above == 1) & (z > 0))
        def _():
            action(-1)

    def x_root(zz, s, src=None):
        piece = half_piece(zz, x, s)
        return send(piece if src is None else src, piece, xr_s.at[zz * SUB + s], xr_r.at[zz * SUB + s], x_peer)

    def quad_piece(index, s):
        return quad_ref.at[index, rows(s), lanes]

    def y_root(index, s, src):
        return send(src, quad_piece(index, s), yr_s.at[index * SUB + s], yr_r.at[index * SUB + s], y_peer)

    def c_half(slot, s, src, dst):
        return send(src, dst, hc_s.at[slot * SUB + s], hc_r.at[slot * SUB + s], c_peer)

    def c_quad(index, s):
        piece = quad_piece(index, s)
        return send(piece, piece, qc_s.at[index * SUB + s], qc_r.at[index * SUB + s], c_peer)

    def spread_on(zz, xx, s, src=None):
        piece = half_piece(zz, xx, s)
        src = piece if src is None else src

        @pl.when(zz // middle == y)
        def _():
            y_root(2 * lax.rem(zz, middle) + xx, s, src).start()

        c_half(2 * zz + xx, s, src, piece).start()

    def z_panel(d):
        return send(panel_ref.at[z_at(d)], own_piece(z, x), zp_s.at[d], zp_r.at[d], at(y, core, z_at(d), x))

    def x_panel(d):
        src = panel_ref.at[z] if d == 0 else own_piece(back(d), x)
        return send(src, own_piece(back(d), x), xp_s.at[d], xp_r.at[d], x_peer)

    my_side = own_ref.at[:, :, pl.ds(pl.multiple_of(x * part, part), part)]

    def side_slot(yy, cc):
        return side_ref.at[2 * yy + cc]

    y_side = send(my_side, side_slot(y, core), yp_s, yp_r, y_peer)
    c_side = [
        send(my_side, side_slot(y, core), pc_s.at[0], pc_r.at[0], c_peer),
        send(side_slot(1 - y, core), side_slot(1 - y, core), pc_s.at[1], pc_r.at[1], c_peer),
    ]

    for d in range(1, slices):
        z_panel(d).start()
    x_panel(0).start()
    for s in range(SUB):

        @pl.when(z < slices - 1)
        def _():
            z_own(0, s).start()

        @pl.when(z > 0)
        def _():
            z_own(1, s).start()

        x_root(z, s, root_piece(s)).start()
        spread_on(z, x, s, root_piece(s))
    local = [pltpu.make_async_copy(root_piece(s), half_piece(z, x, s), loc.at[2 + s]) for s in range(SUB)]
    local.append(pltpu.make_async_copy(panel_ref.at[z], own_piece(z, x), loc.at[1]))
    for copy in local:
        copy.start()
    for d in range(1, slices):
        z_panel(d).wait_recv()
        x_panel(d).start()
    for s in range(SUB):
        x_root(z, s).wait_recv()
        spread_on(z, 1 - x, s)
    local[-1].wait()
    for d in range(slices):
        x_panel(d).wait_recv()
    y_side.start()
    c_side[0].start()
    own_side = pltpu.make_async_copy(my_side, side_slot(y, core), loc.at[0])
    own_side.start()

    upper = z // middle
    folded = z + upper * (slices - 1 - 2 * z)
    sources = []
    for i in range(slices - 1):
        source = i + (i + slices - folded) // slices
        sources.append(source + upper * (slices - 1 - 2 * source))
    for i in range(slices):
        for s in range(SUB):
            if i < slices - 1:
                zz = sources[i]
                send(root_piece(s), half_piece(zz, x, s), zr_s.at[zz * SUB + s], zr_r.at[zz * SUB + s], x_peer).wait_recv()
                when_passed(zz, lambda step: z_pass(zz, s, step).start())
                x_root(zz, s).start()
                spread_on(zz, x, s)
            if i > 0:
                x_root(sources[i - 1], s).wait_recv()
                spread_on(sources[i - 1], 1 - x, s)
    y_side.wait_recv()
    c_side[1].start()
    for index in range(slices):
        for s in range(SUB):
            y_root(index, s, root_piece(s)).wait_recv()
            c_quad(index, s).start()
    for slot in range(2 * slices):
        for s in range(SUB):
            c_half(slot, s, root_piece(s), quad_piece(0, s)).wait()
    for copy in c_side:
        copy.wait()
    for index in range(slices):
        for s in range(SUB):
            c_quad(index, s).wait()
            y_root(index, s, root_piece(s)).wait_send()
            x_root(index, s).wait_send()
    for d in range(slices):
        if d > 0:
            z_panel(d).wait_send()
        x_panel(d).wait_send()
    for s in range(SUB):

        @pl.when(z < slices - 1)
        def _():
            z_own(0, s).wait_send()

        @pl.when(z > 0)
        def _():
            z_own(1, s).wait_send()

        for zz in sources:
            when_passed(zz, lambda step: z_pass(zz, s, step).wait_send())
        local[s].wait()
    y_side.wait_send()
    own_side.wait()


def solve_kernel(slices, list_ref, count_ref, half_ref, quad_ref, own_ref, side_ref, off_ref, schur_ref, spread, product):
    half = half_ref.shape[0] // 2
    tile = 2 * BLOCK
    y, _, z, _ = place(slices)
    blocks = 2 * half // BLOCK
    used = count_ref[z]

    def block_rows(k):
        block = lax.rem(list_ref[z, k] + y * (blocks // 2), blocks)
        return pl.ds(pl.multiple_of(block * BLOCK, BLOCK), BLOCK)

    spread[...] = jnp.zeros_like(spread)
    for k in range(NSMAX):

        @pl.when(k < used)
        def _():
            spread[block_rows(k), :] = own_ref[pl.ds(k * BLOCK, BLOCK), :]

    near, far = spread[:half, :], spread[half:, :]

    def step(t, carry):
        rows = pl.ds(pl.multiple_of(t * tile, tile), tile)
        low = pl.ds(pl.multiple_of(half + t * tile, tile), tile)
        product[rows, :] = jnp.dot(
            half_ref[rows, :], near, preferred_element_type=jnp.float32
        ) + lax.dot_general(
            half_ref[pl.ds(half, half), rows], far, (((0,), (0,)), ((), ())), preferred_element_type=jnp.float32
        )
        product[low, :] = jnp.dot(
            half_ref[low, :], near, preferred_element_type=jnp.float32
        ) + jnp.dot(quad_ref[rows, :], far, preferred_element_type=jnp.float32)
        return carry

    lax.fori_loop(0, half // tile, step, 0)
    for k in range(NSMAX):
        rows = block_rows(k)
        off_ref[pl.ds(k * BLOCK, BLOCK), :] = jnp.where(k < used, -product[rows, :], 0.0).astype(jnp.bfloat16)
    off = off_ref[...]
    for part in range(side_ref.shape[0]):
        schur_ref[part] = lax.dot_general(
            side_ref[part], off, (((0,), (0,)), ((), ())), preferred_element_type=jnp.float32
        ).astype(jnp.bfloat16)


def return_kernel(slices, off_ref, schur_ref, off_out, schur_out, os, orr, ss, sr, loc):
    y, core, z, x = place(slices)

    def target(d):
        return at(y, core, lax.rem(z + d, slices), x)

    greet([target(d) for d in range(1, slices)])
    copies = []
    for d in range(1, slices):
        zz = lax.rem(z + d, slices)
        copies.append(send(off_ref.at[2 * zz + x], off_out.at[z], os.at[d], orr.at[d], target(d)))
    for d in range(1, slices):
        zz = lax.rem(z + d, slices)
        copies.append(send(schur_ref.at[zz], schur_out.at[z], ss.at[d], sr.at[d], target(d)))
    for copy in copies:
        copy.start()
    local = [
        pltpu.make_async_copy(off_ref.at[2 * z + x], off_out.at[z], loc.at[0]),
        pltpu.make_async_copy(schur_ref.at[z], schur_out.at[z], loc.at[1]),
    ]
    for copy in local:
        copy.start()
    for copy in local + copies:
        copy.wait()


def owner_body(slices, root_inverse, lower_panels, struct_blocks, struct_count, diag_inverse):
    vmem = pl.BlockSpec(memory_space=pltpu.VMEM)
    smem = pl.BlockSpec(memory_space=pltpu.SMEM)
    bf16 = jnp.bfloat16
    root_rows, root_cols = root_inverse.shape
    count, local_rows, local_cols = lower_panels.shape
    chunk = 2 * slices
    order = root_rows * chunk
    part = local_cols // 2
    dma = pltpu.SemaphoreType.DMA
    pair = lambda n: [dma((n,)), dma((n,))]
    one = [dma, dma]
    half, quad, own, side = pl.pallas_call(
        functools.partial(gather_kernel, slices),
        out_shape=[
            jax.ShapeDtypeStruct((chunk, root_rows, 2 * root_cols), bf16),
            jax.ShapeDtypeStruct((slices, root_rows, 2 * root_cols), bf16),
            jax.ShapeDtypeStruct((chunk, local_rows, local_cols), bf16),
            jax.ShapeDtypeStruct((4, chunk, local_rows, part), bf16),
        ],
        in_specs=[vmem] * 2,
        out_specs=[vmem] * 4,
        scratch_shapes=[dma((2 * SUB,))]
        + (pair(slices * SUB) + pair(slices)) * 2
        + pair(slices * SUB)
        + one
        + pair(2 * slices * SUB)
        + pair(slices * SUB)
        + pair(2)
        + [dma((2 + SUB,))],
        compiler_params=pltpu.CompilerParams(collective_id=0, has_side_effects=True),
    )(root_inverse, lower_panels)
    packed = chunk * local_rows
    off, schur = pl.pallas_call(
        functools.partial(solve_kernel, slices),
        out_shape=[
            jax.ShapeDtypeStruct((packed, local_cols), bf16),
            jax.ShapeDtypeStruct((4, part, local_cols), bf16),
        ],
        in_specs=[smem] * 2 + [vmem] * 4,
        out_specs=[vmem] * 2,
        scratch_shapes=[pltpu.VMEM((order, local_cols), bf16), pltpu.VMEM((order, local_cols), jnp.float32)],
    )(
        struct_blocks,
        struct_count,
        half.reshape(order, 2 * root_cols),
        quad.reshape(order // 2, 2 * root_cols),
        own.reshape(packed, local_cols),
        side.reshape(4, packed, part),
    )
    offdiag, terms = pl.pallas_call(
        functools.partial(return_kernel, slices),
        out_shape=[
            jax.ShapeDtypeStruct(lower_panels.shape, bf16),
            jax.ShapeDtypeStruct((count, part, local_cols), bf16),
        ],
        in_specs=[vmem] * 2,
        out_specs=[vmem] * 2,
        scratch_shapes=pair(slices) * 2 + [dma((2,))],
        compiler_params=pltpu.CompilerParams(collective_id=1, has_side_effects=True),
    )(off.reshape(chunk, local_rows, local_cols), schur)
    return (offdiag, diag_inverse - terms.astype(jnp.float32))


def spread_body(*arguments):
    rows, cols = lax.axis_size("row"), lax.axis_size("col")
    slices = arguments[1].shape[0]
    if cols == 2 * slices and rows == 4 and slices == 4:
        return owner_body(slices, *arguments)
    return body(*arguments)


def solution(mesh):
    in_specs = (P("col", "row"), P(None, "col", "row"), P(), P(), P(None, "col", "row"))
    out_specs = (P(None, "col", "row"), P(None, "col", "row"))
    return jax.shard_map(spread_body, mesh=mesh, in_specs=in_specs, out_specs=out_specs, check_vma=False)
```

```python
import functools

import jax
import jax.numpy as jnp
from jax import lax
from jax.experimental import pallas as pl
from jax.experimental.pallas import tpu as pltpu
from jax.sharding import PartitionSpec as P

BLOCK = 128
NSMAX = 12


def body(root_inverse, lower_panels, struct_blocks, struct_count, diag_inverse):
    col_index = lax.axis_index("col")
    root_panel = lax.all_gather(root_inverse, "row", axis=1, tiled=True)
    root_width = root_panel.shape[1]
    block_count = root_width // BLOCK
    own_rows = root_panel.shape[0]
    per_dev = own_rows // BLOCK
    local_packed = lower_panels.shape[1]

    def solve_group(lower_group, block_lists, block_counts, inverse_group):
        group_size = lower_group.shape[0]
        cols_here = lower_group.shape[2]
        gathered = lax.all_gather(lower_group, "col", axis=1, tiled=True)
        packed_total = gathered.shape[1]
        full_mask = jnp.arange(packed_total)[None, :] // BLOCK < block_counts[:, None]
        gathered = gathered * full_mask[:, :, None].astype(jnp.bfloat16)
        in_use = jnp.arange(NSMAX)[None, :] < block_counts[:, None]
        onehot = (
            (block_lists[:, None, :] == jnp.arange(block_count)[None, :, None]) & in_use[:, None, :]
        ).astype(jnp.bfloat16)
        spread = jnp.einsum(
            "gbk,gkic->gbic",
            onehot,
            gathered.reshape(group_size, NSMAX, BLOCK, cols_here),
            preferred_element_type=jnp.float32,
        )
        spread = spread.astype(jnp.bfloat16).reshape(group_size, root_width, cols_here)
        root_part = -jnp.einsum(
            "rw,gwc->grc", root_panel, spread, preferred_element_type=jnp.float32
        )
        packed_index = col_index * local_packed + jnp.arange(local_packed)
        local_mask = packed_index[None, :] // BLOCK < block_counts[:, None]
        own_select = lax.dynamic_slice_in_dim(onehot, col_index * per_dev, per_dev, 1).astype(
            jnp.float32
        )
        selected = jnp.einsum(
            "gjk,gjic->gkic",
            own_select,
            root_part.reshape(group_size, per_dev, BLOCK, cols_here),
            precision=lax.Precision.HIGHEST,
            preferred_element_type=jnp.float32,
        )
        selected = selected.reshape(group_size, packed_total, cols_here)
        offdiag = lax.psum_scatter(
            selected.astype(jnp.bfloat16), "col", scatter_dimension=1, tiled=True
        )
        full_cols = lax.all_gather(lower_group, "row", axis=2, tiled=True)
        masked_rows = full_cols * local_mask[:, :, None].astype(jnp.bfloat16)
        schur_terms = jnp.einsum(
            "gka,gkc->gac", masked_rows, offdiag, preferred_element_type=jnp.float32
        )
        schur_part = lax.psum_scatter(
            schur_terms.astype(jnp.bfloat16), "col", scatter_dimension=1, tiled=True
        ).astype(jnp.float32)
        return (offdiag, inverse_group - schur_part)

    group_size = 4
    turn_count = lower_panels.shape[0] // group_size

    def regroup(source_array):
        return source_array.reshape((turn_count, group_size) + source_array.shape[1:])

    def one_turn(running, inputs_now):
        return (running, solve_group(*inputs_now))

    finished, outputs = lax.scan(
        one_turn,
        jnp.int32(0),
        (
            regroup(lower_panels),
            regroup(struct_blocks),
            regroup(struct_count),
            regroup(diag_inverse),
        ),
    )
    offdiag_all, diag_all = outputs
    return (offdiag_all.reshape(lower_panels.shape), diag_all.reshape(diag_inverse.shape))


def place(slices):
    row, col = lax.axis_index("row"), lax.axis_index("col")
    return row // 2, row % 2, col // 2, col % 2


def at(y, core, z, x):
    return {"row": 2 * y + core, "col": 2 * z + x}


def greet(peers):
    barrier = pltpu.get_barrier_semaphore()
    for peer in peers:
        pl.semaphore_signal(barrier, inc=1, device_id=peer, device_id_type=pl.DeviceIdType.MESH)
    pl.semaphore_wait(barrier, len(peers))


def send(src, dst, send_sem, recv_sem, device):
    return pltpu.make_async_remote_copy(
        src_ref=src,
        dst_ref=dst,
        send_sem=send_sem,
        recv_sem=recv_sem,
        device_id=device,
        device_id_type=pl.DeviceIdType.MESH,
    )


SUB = 2


def gather_kernel(slices, root_ref, panel_ref, half_ref, quad_ref, own_ref, side_ref, *sems):
    (zo_s, zr_s, zr_r, zp_s, zp_r, xr_s, xr_r, xp_s, xp_r, yr_s, yr_r, yp_s, yp_r, hc_s, hc_r, qc_s, qc_r, pc_s, pc_r, loc) = sems
    y, core, z, x = place(slices)
    height, width = root_ref.shape[0] // SUB, root_ref.shape[1]
    chunk = 2 * slices
    middle = slices // 2
    lanes = pl.ds(pl.multiple_of(core * width, width), width)
    part = side_ref.shape[3]
    x_peer, y_peer, c_peer = at(y, core, z, 1 - x), at(1 - y, core, z, x), at(y, 1 - core, z, x)

    def z_at(d):
        return lax.rem(z + d, slices)

    def back(d):
        return lax.rem(z + slices - d, slices)

    greet([at(y, core, z_at(d), x) for d in range(1, slices)] + [x_peer, y_peer, c_peer])

    def rows(s):
        return pl.ds(s * height, height)

    def root_piece(s):
        return root_ref.at[rows(s)]

    def half_piece(zz, xx, s):
        return half_ref.at[lax.rem(2 * zz + xx + slices * y, chunk), rows(s), lanes]

    def own_piece(zz, xx):
        return own_ref.at[2 * zz + xx]

    def z_own(way, s):
        step = 1 - 2 * way
        return send(
            root_piece(s), half_piece(z, x, s), zo_s.at[way * SUB + s], zr_r.at[z * SUB + s], at(y, core, z + step, x)
        )

    def z_pass(zz, s, step):
        piece = half_piece(zz, x, s)
        return send(piece, piece, zr_s.at[zz * SUB + s], zr_r.at[zz * SUB + s], at(y, core, z + step, x))

    def when_passed(zz, action):
        above = (zz + slices - z) // slices

        @pl.when((above == 0) & (z < slices - 1))
        def _():
            action(1)

        @pl.when((above == 1) & (z > 0))
        def _():
            action(-1)

    def x_root(zz, s, src=None):
        piece = half_piece(zz, x, s)
        return send(piece if src is None else src, piece, xr_s.at[zz * SUB + s], xr_r.at[zz * SUB + s], x_peer)

    def quad_piece(index, s):
        return quad_ref.at[index, rows(s), lanes]

    def y_root(index, s, src):
        return send(src, quad_piece(index, s), yr_s.at[index * SUB + s], yr_r.at[index * SUB + s], y_peer)

    def c_half(slot, s, src, dst):
        return send(src, dst, hc_s.at[slot * SUB + s], hc_r.at[slot * SUB + s], c_peer)

    def c_quad(index, s):
        piece = quad_piece(index, s)
        return send(piece, piece, qc_s.at[index * SUB + s], qc_r.at[index * SUB + s], c_peer)

    def spread_on(zz, xx, s, src=None):
        piece = half_piece(zz, xx, s)
        src = piece if src is None else src

        @pl.when(zz // middle == y)
        def _():
            y_root(2 * lax.rem(zz, middle) + xx, s, src).start()

        c_half(2 * zz + xx, s, src, piece).start()

    def z_panel(d):
        return send(panel_ref.at[z_at(d)], own_piece(z, x), zp_s.at[d], zp_r.at[d], at(y, core, z_at(d), x))

    def x_panel(d):
        src = panel_ref.at[z] if d == 0 else own_piece(back(d), x)
        return send(src, own_piece(back(d), x), xp_s.at[d], xp_r.at[d], x_peer)

    my_side = own_ref.at[:, :, pl.ds(pl.multiple_of(x * part, part), part)]

    def side_slot(yy, cc):
        return side_ref.at[2 * yy + cc]

    y_side = send(my_side, side_slot(y, core), yp_s, yp_r, y_peer)
    c_side = [
        send(my_side, side_slot(y, core), pc_s.at[0], pc_r.at[0], c_peer),
        send(side_slot(1 - y, core), side_slot(1 - y, core), pc_s.at[1], pc_r.at[1], c_peer),
    ]

    for d in range(1, slices):
        z_panel(d).start()
    x_panel(0).start()
    for s in range(SUB):

        @pl.when(z < slices - 1)
        def _():
            z_own(0, s).start()

        @pl.when(z > 0)
        def _():
            z_own(1, s).start()

        x_root(z, s, root_piece(s)).start()
        spread_on(z, x, s, root_piece(s))
    local = [pltpu.make_async_copy(root_piece(s), half_piece(z, x, s), loc.at[2 + s]) for s in range(SUB)]
    local.append(pltpu.make_async_copy(panel_ref.at[z], own_piece(z, x), loc.at[1]))
    for copy in local:
        copy.start()
    for d in range(1, slices):
        z_panel(d).wait_recv()
        x_panel(d).start()
    for s in range(SUB):
        x_root(z, s).wait_recv()
        spread_on(z, 1 - x, s)
    local[-1].wait()
    for d in range(slices):
        x_panel(d).wait_recv()
    y_side.start()
    c_side[0].start()
    own_side = pltpu.make_async_copy(my_side, side_slot(y, core), loc.at[0])
    own_side.start()

    upper = z // middle
    folded = z + upper * (slices - 1 - 2 * z)
    sources = []
    for i in range(slices - 1):
        source = i + (i + slices - folded) // slices
        sources.append(source + upper * (slices - 1 - 2 * source))
    for i in range(slices):
        for s in range(SUB):
            if i < slices - 1:
                zz = sources[i]
                send(root_piece(s), half_piece(zz, x, s), zr_s.at[zz * SUB + s], zr_r.at[zz * SUB + s], x_peer).wait_recv()
                when_passed(zz, lambda step: z_pass(zz, s, step).start())
                x_root(zz, s).start()
                spread_on(zz, x, s)
            if i > 0:
                x_root(sources[i - 1], s).wait_recv()
                spread_on(sources[i - 1], 1 - x, s)
    y_side.wait_recv()
    c_side[1].start()
    for index in range(slices):
        for s in range(SUB):
            y_root(index, s, root_piece(s)).wait_recv()
            c_quad(index, s).start()
    for slot in range(2 * slices):
        for s in range(SUB):
            c_half(slot, s, root_piece(s), quad_piece(0, s)).wait()
    for copy in c_side:
        copy.wait()
    for index in range(slices):
        for s in range(SUB):
            c_quad(index, s).wait()
            y_root(index, s, root_piece(s)).wait_send()
            x_root(index, s).wait_send()
    for d in range(slices):
        if d > 0:
            z_panel(d).wait_send()
        x_panel(d).wait_send()
    for s in range(SUB):

        @pl.when(z < slices - 1)
        def _():
            z_own(0, s).wait_send()

        @pl.when(z > 0)
        def _():
            z_own(1, s).wait_send()

        for zz in sources:
            when_passed(zz, lambda step: z_pass(zz, s, step).wait_send())
        local[s].wait()
    y_side.wait_send()
    own_side.wait()


def solve_kernel(slices, list_ref, count_ref, half_ref, quad_ref, own_ref, side_ref, off_ref, schur_ref, spread, product):
    half = half_ref.shape[0] // 2
    tile = 2 * BLOCK
    y, _, z, _ = place(slices)
    blocks = 2 * half // BLOCK
    used = count_ref[z]

    def block_rows(k):
        block = lax.rem(list_ref[z, k] + y * (blocks // 2), blocks)
        return pl.ds(pl.multiple_of(block * BLOCK, BLOCK), BLOCK)

    spread[...] = jnp.zeros_like(spread)
    for k in range(NSMAX):

        @pl.when(k < used)
        def _():
            spread[block_rows(k), :] = own_ref[pl.ds(k * BLOCK, BLOCK), :]

    near, far = spread[:half, :], spread[half:, :]

    def step(t, carry):
        rows = pl.ds(pl.multiple_of(t * tile, tile), tile)
        low = pl.ds(pl.multiple_of(half + t * tile, tile), tile)
        product[rows, :] = jnp.dot(
            half_ref[rows, :], near, preferred_element_type=jnp.float32
        ) + lax.dot_general(
            half_ref[pl.ds(half, half), rows], far, (((0,), (0,)), ((), ())), preferred_element_type=jnp.float32
        )
        product[low, :] = jnp.dot(
            half_ref[low, :], near, preferred_element_type=jnp.float32
        ) + jnp.dot(quad_ref[rows, :], far, preferred_element_type=jnp.float32)
        return carry

    lax.fori_loop(0, half // tile, step, 0)
    for k in range(NSMAX):
        rows = block_rows(k)
        off_ref[pl.ds(k * BLOCK, BLOCK), :] = jnp.where(k < used, -product[rows, :], 0.0).astype(jnp.bfloat16)
    off = off_ref[...]
    for part in range(side_ref.shape[0]):
        schur_ref[part] = lax.dot_general(
            side_ref[part], off, (((0,), (0,)), ((), ())), preferred_element_type=jnp.float32
        ).astype(jnp.bfloat16)


def return_kernel(slices, off_ref, schur_ref, off_out, schur_out, os, orr, ss, sr, loc):
    y, core, z, x = place(slices)

    def target(d):
        return at(y, core, lax.rem(z + d, slices), x)

    greet([target(d) for d in range(1, slices)])
    copies = []
    for d in range(1, slices):
        zz = lax.rem(z + d, slices)
        copies.append(send(off_ref.at[2 * zz + x], off_out.at[z], os.at[d], orr.at[d], target(d)))
    for d in range(1, slices):
        zz = lax.rem(z + d, slices)
        copies.append(send(schur_ref.at[zz], schur_out.at[z], ss.at[d], sr.at[d], target(d)))
    for copy in copies:
        copy.start()
    local = [
        pltpu.make_async_copy(off_ref.at[2 * z + x], off_out.at[z], loc.at[0]),
        pltpu.make_async_copy(schur_ref.at[z], schur_out.at[z], loc.at[1]),
    ]
    for copy in local:
        copy.start()
    for copy in local + copies:
        copy.wait()


def owner_body(slices, root_inverse, lower_panels, struct_blocks, struct_count, diag_inverse):
    vmem = pl.BlockSpec(memory_space=pltpu.VMEM)
    smem = pl.BlockSpec(memory_space=pltpu.SMEM)
    bf16 = jnp.bfloat16
    root_rows, root_cols = root_inverse.shape
    count, local_rows, local_cols = lower_panels.shape
    chunk = 2 * slices
    order = root_rows * chunk
    part = local_cols // 2
    grant = 24 * 2**20
    dma = pltpu.SemaphoreType.DMA
    pair = lambda n: [dma((n,)), dma((n,))]
    one = [dma, dma]
    half, quad, own, side = pl.pallas_call(
        functools.partial(gather_kernel, slices),
        out_shape=[
            jax.ShapeDtypeStruct((chunk, root_rows, 2 * root_cols), bf16),
            jax.ShapeDtypeStruct((slices, root_rows, 2 * root_cols), bf16),
            jax.ShapeDtypeStruct((chunk, local_rows, local_cols), bf16),
            jax.ShapeDtypeStruct((4, chunk, local_rows, part), bf16),
        ],
        in_specs=[vmem] * 2,
        out_specs=[vmem] * 4,
        scratch_shapes=[dma((2 * SUB,))]
        + (pair(slices * SUB) + pair(slices)) * 2
        + pair(slices * SUB)
        + one
        + pair(2 * slices * SUB)
        + pair(slices * SUB)
        + pair(2)
        + [dma((2 + SUB,))],
        compiler_params=pltpu.CompilerParams(collective_id=0, has_side_effects=True, vmem_limit_bytes=grant),
    )(root_inverse, lower_panels)
    packed = chunk * local_rows
    off, schur = pl.pallas_call(
        functools.partial(solve_kernel, slices),
        out_shape=[
            jax.ShapeDtypeStruct((packed, local_cols), bf16),
            jax.ShapeDtypeStruct((4, part, local_cols), bf16),
        ],
        in_specs=[smem] * 2 + [vmem] * 4,
        out_specs=[vmem] * 2,
        scratch_shapes=[pltpu.VMEM((order, local_cols), bf16), pltpu.VMEM((order, local_cols), jnp.float32)],
        compiler_params=pltpu.CompilerParams(vmem_limit_bytes=grant),
    )(
        struct_blocks,
        struct_count,
        half.reshape(order, 2 * root_cols),
        quad.reshape(order // 2, 2 * root_cols),
        own.reshape(packed, local_cols),
        side.reshape(4, packed, part),
    )
    offdiag, terms = pl.pallas_call(
        functools.partial(return_kernel, slices),
        out_shape=[
            jax.ShapeDtypeStruct(lower_panels.shape, bf16),
            jax.ShapeDtypeStruct((count, part, local_cols), bf16),
        ],
        in_specs=[vmem] * 2,
        out_specs=[vmem] * 2,
        scratch_shapes=pair(slices) * 2 + [dma((2,))],
        compiler_params=pltpu.CompilerParams(collective_id=1, has_side_effects=True, vmem_limit_bytes=grant),
    )(off.reshape(chunk, local_rows, local_cols), schur)
    return (offdiag, diag_inverse - terms.astype(jnp.float32))


def spread_body(*arguments):
    rows, cols = lax.axis_size("row"), lax.axis_size("col")
    slices = arguments[1].shape[0]
    if cols == 2 * slices and rows == 4 and slices == 4:
        return owner_body(slices, *arguments)
    return body(*arguments)


def solution(mesh):
    in_specs = (P("col", "row"), P(None, "col", "row"), P(), P(), P(None, "col", "row"))
    out_specs = (P(None, "col", "row"), P(None, "col", "row"))
    return jax.shard_map(spread_body, mesh=mesh, in_specs=in_specs, out_specs=out_specs, check_vma=False)
```

```python
import functools

import jax
import jax.numpy as jnp
from jax import lax
from jax.experimental import pallas as pl
from jax.experimental.pallas import tpu as pltpu
from jax.sharding import PartitionSpec as P

BLOCK = 128
NSMAX = 12


def body(root_inverse, lower_panels, struct_blocks, struct_count, diag_inverse):
    col_index = lax.axis_index("col")
    root_panel = lax.all_gather(root_inverse, "row", axis=1, tiled=True)
    root_width = root_panel.shape[1]
    block_count = root_width // BLOCK
    own_rows = root_panel.shape[0]
    per_dev = own_rows // BLOCK
    local_packed = lower_panels.shape[1]

    def solve_group(lower_group, block_lists, block_counts, inverse_group):
        group_size = lower_group.shape[0]
        cols_here = lower_group.shape[2]
        gathered = lax.all_gather(lower_group, "col", axis=1, tiled=True)
        packed_total = gathered.shape[1]
        full_mask = jnp.arange(packed_total)[None, :] // BLOCK < block_counts[:, None]
        gathered = gathered * full_mask[:, :, None].astype(jnp.bfloat16)
        in_use = jnp.arange(NSMAX)[None, :] < block_counts[:, None]
        onehot = (
            (block_lists[:, None, :] == jnp.arange(block_count)[None, :, None]) & in_use[:, None, :]
        ).astype(jnp.bfloat16)
        spread = jnp.einsum(
            "gbk,gkic->gbic",
            onehot,
            gathered.reshape(group_size, NSMAX, BLOCK, cols_here),
            preferred_element_type=jnp.float32,
        )
        spread = spread.astype(jnp.bfloat16).reshape(group_size, root_width, cols_here)
        root_part = -jnp.einsum(
            "rw,gwc->grc", root_panel, spread, preferred_element_type=jnp.float32
        )
        packed_index = col_index * local_packed + jnp.arange(local_packed)
        local_mask = packed_index[None, :] // BLOCK < block_counts[:, None]
        own_select = lax.dynamic_slice_in_dim(onehot, col_index * per_dev, per_dev, 1).astype(
            jnp.float32
        )
        selected = jnp.einsum(
            "gjk,gjic->gkic",
            own_select,
            root_part.reshape(group_size, per_dev, BLOCK, cols_here),
            precision=lax.Precision.HIGHEST,
            preferred_element_type=jnp.float32,
        )
        selected = selected.reshape(group_size, packed_total, cols_here)
        offdiag = lax.psum_scatter(
            selected.astype(jnp.bfloat16), "col", scatter_dimension=1, tiled=True
        )
        full_cols = lax.all_gather(lower_group, "row", axis=2, tiled=True)
        masked_rows = full_cols * local_mask[:, :, None].astype(jnp.bfloat16)
        schur_terms = jnp.einsum(
            "gka,gkc->gac", masked_rows, offdiag, preferred_element_type=jnp.float32
        )
        schur_part = lax.psum_scatter(
            schur_terms.astype(jnp.bfloat16), "col", scatter_dimension=1, tiled=True
        ).astype(jnp.float32)
        return (offdiag, inverse_group - schur_part)

    group_size = 4
    turn_count = lower_panels.shape[0] // group_size

    def regroup(source_array):
        return source_array.reshape((turn_count, group_size) + source_array.shape[1:])

    def one_turn(running, inputs_now):
        return (running, solve_group(*inputs_now))

    finished, outputs = lax.scan(
        one_turn,
        jnp.int32(0),
        (
            regroup(lower_panels),
            regroup(struct_blocks),
            regroup(struct_count),
            regroup(diag_inverse),
        ),
    )
    offdiag_all, diag_all = outputs
    return (offdiag_all.reshape(lower_panels.shape), diag_all.reshape(diag_inverse.shape))


def place(slices):
    row, col = lax.axis_index("row"), lax.axis_index("col")
    return row // 2, row % 2, col // 2, col % 2


def at(y, core, z, x):
    return {"row": 2 * y + core, "col": 2 * z + x}


def greet(peers):
    barrier = pltpu.get_barrier_semaphore()
    for peer in peers:
        pl.semaphore_signal(barrier, inc=1, device_id=peer, device_id_type=pl.DeviceIdType.MESH)
    pl.semaphore_wait(barrier, len(peers))


def send(src, dst, send_sem, recv_sem, device):
    return pltpu.make_async_remote_copy(
        src_ref=src,
        dst_ref=dst,
        send_sem=send_sem,
        recv_sem=recv_sem,
        device_id=device,
        device_id_type=pl.DeviceIdType.MESH,
    )


SUB = 2


def gather_kernel(slices, root_ref, panel_ref, half_ref, quad_ref, own_ref, side_ref, *sems):
    (zo_s, zr_s, zr_r, zp_s, zp_r, xr_s, xr_r, xp_s, xp_r, yr_s, yr_r, yp_s, yp_r, hc_s, hc_r, qc_s, qc_r, pc_s, pc_r, loc) = sems
    y, core, z, x = place(slices)
    height, width = root_ref.shape[0] // SUB, root_ref.shape[1]
    chunk = 2 * slices
    middle = slices // 2
    lanes = pl.ds(pl.multiple_of(core * width, width), width)
    part = side_ref.shape[3]
    x_peer, y_peer, c_peer = at(y, core, z, 1 - x), at(1 - y, core, z, x), at(y, 1 - core, z, x)

    def z_at(d):
        return lax.rem(z + d, slices)

    def back(d):
        return lax.rem(z + slices - d, slices)

    greet([at(y, core, z_at(d), x) for d in range(1, slices)] + [x_peer, y_peer, c_peer])

    def rows(s):
        return pl.ds(s * height, height)

    def root_piece(s):
        return root_ref.at[rows(s)]

    def half_piece(zz, xx, s):
        return half_ref.at[lax.rem(2 * zz + xx + slices * y, chunk), rows(s), lanes]

    def own_piece(zz, xx):
        return own_ref.at[2 * zz + xx]

    def z_own(way, s):
        step = 1 - 2 * way
        return send(
            root_piece(s), half_piece(z, x, s), zo_s.at[way * SUB + s], zr_r.at[z * SUB + s], at(y, core, z + step, x)
        )

    def z_pass(zz, s, step):
        piece = half_piece(zz, x, s)
        return send(piece, piece, zr_s.at[zz * SUB + s], zr_r.at[zz * SUB + s], at(y, core, z + step, x))

    def when_passed(zz, action):
        above = (zz + slices - z) // slices

        @pl.when((above == 0) & (z < slices - 1))
        def _():
            action(1)

        @pl.when((above == 1) & (z > 0))
        def _():
            action(-1)

    def x_root(zz, s, src=None):
        piece = half_piece(zz, x, s)
        return send(piece if src is None else src, piece, xr_s.at[zz * SUB + s], xr_r.at[zz * SUB + s], x_peer)

    def quad_piece(index, s):
        return quad_ref.at[index, rows(s), lanes]

    def y_root(index, s, src):
        return send(src, quad_piece(index, s), yr_s.at[index * SUB + s], yr_r.at[index * SUB + s], y_peer)

    def c_half(slot, s, src, dst):
        return send(src, dst, hc_s.at[slot * SUB + s], hc_r.at[slot * SUB + s], c_peer)

    def c_quad(index, s):
        piece = quad_piece(index, s)
        return send(piece, piece, qc_s.at[index * SUB + s], qc_r.at[index * SUB + s], c_peer)

    def spread_on(zz, xx, s, src=None):
        piece = half_piece(zz, xx, s)
        src = piece if src is None else src

        @pl.when(zz // middle == y)
        def _():
            y_root(2 * lax.rem(zz, middle) + xx, s, src).start()

        c_half(2 * zz + xx, s, src, piece).start()

    def z_panel(d):
        return send(panel_ref.at[z_at(d)], own_piece(z, x), zp_s.at[d], zp_r.at[d], at(y, core, z_at(d), x))

    def x_panel(d):
        src = panel_ref.at[z] if d == 0 else own_piece(back(d), x)
        return send(src, own_piece(back(d), x), xp_s.at[d], xp_r.at[d], x_peer)

    my_side = own_ref.at[:, :, pl.ds(pl.multiple_of(x * part, part), part)]

    def side_slot(yy, cc):
        return side_ref.at[2 * yy + cc]

    y_side = send(my_side, side_slot(y, core), yp_s, yp_r, y_peer)
    c_side = [
        send(my_side, side_slot(y, core), pc_s.at[0], pc_r.at[0], c_peer),
        send(side_slot(1 - y, core), side_slot(1 - y, core), pc_s.at[1], pc_r.at[1], c_peer),
    ]

    for s in range(SUB):

        @pl.when(z < slices - 1)
        def _():
            z_own(0, s).start()

        @pl.when(z > 0)
        def _():
            z_own(1, s).start()

        x_root(z, s, root_piece(s)).start()
        spread_on(z, x, s, root_piece(s))
    for d in range(1, slices):
        z_panel(d).start()
    x_panel(0).start()
    local = [pltpu.make_async_copy(root_piece(s), half_piece(z, x, s), loc.at[2 + s]) for s in range(SUB)]
    local.append(pltpu.make_async_copy(panel_ref.at[z], own_piece(z, x), loc.at[1]))
    for copy in local:
        copy.start()
    for s in range(SUB):
        x_root(z, s).wait_recv()
        spread_on(z, 1 - x, s)
    for d in range(1, slices):
        z_panel(d).wait_recv()
        x_panel(d).start()
    local[-1].wait()
    for d in range(slices):
        x_panel(d).wait_recv()
    y_side.start()
    c_side[0].start()
    own_side = pltpu.make_async_copy(my_side, side_slot(y, core), loc.at[0])
    own_side.start()

    upper = z // middle
    folded = z + upper * (slices - 1 - 2 * z)
    sources = []
    for i in range(slices - 1):
        source = i + (i + slices - folded) // slices
        sources.append(source + upper * (slices - 1 - 2 * source))
    for i in range(slices):
        for s in range(SUB):
            if i < slices - 1:
                zz = sources[i]
                send(root_piece(s), half_piece(zz, x, s), zr_s.at[zz * SUB + s], zr_r.at[zz * SUB + s], x_peer).wait_recv()
                when_passed(zz, lambda step: z_pass(zz, s, step).start())
                x_root(zz, s).start()
                spread_on(zz, x, s)
            if i > 0:
                x_root(sources[i - 1], s).wait_recv()
                spread_on(sources[i - 1], 1 - x, s)
    y_side.wait_recv()
    c_side[1].start()
    for index in range(slices):
        for s in range(SUB):
            y_root(index, s, root_piece(s)).wait_recv()
            c_quad(index, s).start()
    for slot in range(2 * slices):
        for s in range(SUB):
            c_half(slot, s, root_piece(s), quad_piece(0, s)).wait()
    for copy in c_side:
        copy.wait()
    for index in range(slices):
        for s in range(SUB):
            c_quad(index, s).wait()
            y_root(index, s, root_piece(s)).wait_send()
            x_root(index, s).wait_send()
    for d in range(slices):
        if d > 0:
            z_panel(d).wait_send()
        x_panel(d).wait_send()
    for s in range(SUB):

        @pl.when(z < slices - 1)
        def _():
            z_own(0, s).wait_send()

        @pl.when(z > 0)
        def _():
            z_own(1, s).wait_send()

        for zz in sources:
            when_passed(zz, lambda step: z_pass(zz, s, step).wait_send())
        local[s].wait()
    y_side.wait_send()
    own_side.wait()


def solve_kernel(slices, list_ref, count_ref, half_ref, quad_ref, own_ref, side_ref, off_ref, schur_ref, spread, product):
    half = half_ref.shape[0] // 2
    tile = 2 * BLOCK
    y, _, z, _ = place(slices)
    blocks = 2 * half // BLOCK
    used = count_ref[z]

    def block_rows(k):
        block = lax.rem(list_ref[z, k] + y * (blocks // 2), blocks)
        return pl.ds(pl.multiple_of(block * BLOCK, BLOCK), BLOCK)

    spread[...] = jnp.zeros_like(spread)
    for k in range(NSMAX):

        @pl.when(k < used)
        def _():
            spread[block_rows(k), :] = own_ref[pl.ds(k * BLOCK, BLOCK), :]

    near, far = spread[:half, :], spread[half:, :]

    def step(t, carry):
        rows = pl.ds(pl.multiple_of(t * tile, tile), tile)
        low = pl.ds(pl.multiple_of(half + t * tile, tile), tile)
        product[rows, :] = jnp.dot(
            half_ref[rows, :], near, preferred_element_type=jnp.float32
        ) + lax.dot_general(
            half_ref[pl.ds(half, half), rows], far, (((0,), (0,)), ((), ())), preferred_element_type=jnp.float32
        )
        product[low, :] = jnp.dot(
            half_ref[low, :], near, preferred_element_type=jnp.float32
        ) + jnp.dot(quad_ref[rows, :], far, preferred_element_type=jnp.float32)
        return carry

    lax.fori_loop(0, half // tile, step, 0)
    for k in range(NSMAX):
        rows = block_rows(k)
        off_ref[pl.ds(k * BLOCK, BLOCK), :] = jnp.where(k < used, -product[rows, :], 0.0).astype(jnp.bfloat16)
    off = off_ref[...]
    for part in range(side_ref.shape[0]):
        schur_ref[part] = lax.dot_general(
            side_ref[part], off, (((0,), (0,)), ((), ())), preferred_element_type=jnp.float32
        ).astype(jnp.bfloat16)


def return_kernel(slices, off_ref, schur_ref, off_out, schur_out, os, orr, ss, sr, loc):
    y, core, z, x = place(slices)

    def target(d):
        return at(y, core, lax.rem(z + d, slices), x)

    greet([target(d) for d in range(1, slices)])
    copies = []
    for d in range(1, slices):
        zz = lax.rem(z + d, slices)
        copies.append(send(off_ref.at[2 * zz + x], off_out.at[z], os.at[d], orr.at[d], target(d)))
    for d in range(1, slices):
        zz = lax.rem(z + d, slices)
        copies.append(send(schur_ref.at[zz], schur_out.at[z], ss.at[d], sr.at[d], target(d)))
    for copy in copies:
        copy.start()
    local = [
        pltpu.make_async_copy(off_ref.at[2 * z + x], off_out.at[z], loc.at[0]),
        pltpu.make_async_copy(schur_ref.at[z], schur_out.at[z], loc.at[1]),
    ]
    for copy in local:
        copy.start()
    for copy in local + copies:
        copy.wait()


def owner_body(slices, root_inverse, lower_panels, struct_blocks, struct_count, diag_inverse):
    vmem = pl.BlockSpec(memory_space=pltpu.VMEM)
    smem = pl.BlockSpec(memory_space=pltpu.SMEM)
    bf16 = jnp.bfloat16
    root_rows, root_cols = root_inverse.shape
    count, local_rows, local_cols = lower_panels.shape
    chunk = 2 * slices
    order = root_rows * chunk
    part = local_cols // 2
    grant = 24 * 2**20
    dma = pltpu.SemaphoreType.DMA
    pair = lambda n: [dma((n,)), dma((n,))]
    one = [dma, dma]
    half, quad, own, side = pl.pallas_call(
        functools.partial(gather_kernel, slices),
        out_shape=[
            jax.ShapeDtypeStruct((chunk, root_rows, 2 * root_cols), bf16),
            jax.ShapeDtypeStruct((slices, root_rows, 2 * root_cols), bf16),
            jax.ShapeDtypeStruct((chunk, local_rows, local_cols), bf16),
            jax.ShapeDtypeStruct((4, chunk, local_rows, part), bf16),
        ],
        in_specs=[vmem] * 2,
        out_specs=[vmem] * 4,
        scratch_shapes=[dma((2 * SUB,))]
        + (pair(slices * SUB) + pair(slices)) * 2
        + pair(slices * SUB)
        + one
        + pair(2 * slices * SUB)
        + pair(slices * SUB)
        + pair(2)
        + [dma((2 + SUB,))],
        compiler_params=pltpu.CompilerParams(collective_id=0, has_side_effects=True, vmem_limit_bytes=grant),
    )(root_inverse, lower_panels)
    packed = chunk * local_rows
    off, schur = pl.pallas_call(
        functools.partial(solve_kernel, slices),
        out_shape=[
            jax.ShapeDtypeStruct((packed, local_cols), bf16),
            jax.ShapeDtypeStruct((4, part, local_cols), bf16),
        ],
        in_specs=[smem] * 2 + [vmem] * 4,
        out_specs=[vmem] * 2,
        scratch_shapes=[pltpu.VMEM((order, local_cols), bf16), pltpu.VMEM((order, local_cols), jnp.float32)],
        compiler_params=pltpu.CompilerParams(vmem_limit_bytes=grant),
    )(
        struct_blocks,
        struct_count,
        half.reshape(order, 2 * root_cols),
        quad.reshape(order // 2, 2 * root_cols),
        own.reshape(packed, local_cols),
        side.reshape(4, packed, part),
    )
    offdiag, terms = pl.pallas_call(
        functools.partial(return_kernel, slices),
        out_shape=[
            jax.ShapeDtypeStruct(lower_panels.shape, bf16),
            jax.ShapeDtypeStruct((count, part, local_cols), bf16),
        ],
        in_specs=[vmem] * 2,
        out_specs=[vmem] * 2,
        scratch_shapes=pair(slices) * 2 + [dma((2,))],
        compiler_params=pltpu.CompilerParams(collective_id=1, has_side_effects=True, vmem_limit_bytes=grant),
    )(off.reshape(chunk, local_rows, local_cols), schur)
    return (offdiag, diag_inverse - terms.astype(jnp.float32))


def spread_body(*arguments):
    rows, cols = lax.axis_size("row"), lax.axis_size("col")
    slices = arguments[1].shape[0]
    if cols == 2 * slices and rows == 4 and slices == 4:
        return owner_body(slices, *arguments)
    return body(*arguments)


def solution(mesh):
    in_specs = (P("col", "row"), P(None, "col", "row"), P(), P(), P(None, "col", "row"))
    out_specs = (P(None, "col", "row"), P(None, "col", "row"))
    return jax.shard_map(spread_body, mesh=mesh, in_specs=in_specs, out_specs=out_specs, check_vma=False)
```
